512 devices in a mesh: gx: 8 (over x, core), gy: 4 (over y), gz: 16 (over z).
Axes of the slice: x: 4, y: 4, z: 16, core: 2. Of those that a mesh axis runs over, the one named last changes fastest.
Arguments:
- residual: bfloat16 [8, 4, 16, 3, 256, 256], P('gx', 'gy', 'gz'), may hold values from -6 to 6
- face_basis: bfloat16 [8, 4, 16, 3, 256, 256], P('gx', 'gy', 'gz'), may hold values from -0.375 to 0.375
- factor: bfloat16 [8, 4, 16, 768, 768], P('gx', 'gy', 'gz'), may hold values from -0.21875 to 0.21875
- coarse_inv: bfloat16 [8, 4, 16, 768, 768], P('gx', 'gy', 'gz'), may hold values from -0.21875 to 0.21875
- item_owner: int32 [8, 4, 16, 24], P('gx', 'gy', 'gz'), may hold values from 0 to 15, as said below
Outputs:
- result: bfloat16 [8, 4, 16, 3, 256, 256], P('gx', 'gy', 'gz')
The draws below stay inside these ranges and needn't reach their ends.
Inputs may be any that keep to these rules, and one draw needn't show every extreme that they name: `item_owner`: within the groups of one subdomain, at most 3 name the same owner, and in every subdomain some owner is named exactly 3 times.
All inputs are finite; a program needn't handle non-finite values.
Results may differ from the reference program's by a relative error of at most 0.006.
Values may be sent and summed in bfloat16 or wider, within the bound.
A program may use at most 64 MiB of HBM per device.

```python
import jax
import jax.numpy as jnp
from jax import lax

R = 256
FACE = 256
PF = 128
GROUP = 16
ITEMS = 24
SEND_CAP = 3
DF = 128
SOLVE = 768
CS = 768
N_GX = 8
N_GY = 4
N_GZ = 16


def draw_item_owner(key, part):
    slot_total = SEND_CAP * N_GZ
    key_popular, key_owner, key_slot, key_shuffle = jax.random.split(jax.random.fold_in(key, 17), 4)
    grid_shape = (N_GX, N_GY, N_GZ)
    popular = jax.random.randint(key_popular, (N_GX, N_GY, 1, N_GZ), 0, 4) == 0
    owner_score = jax.random.randint(key_owner, grid_shape + (N_GZ,), 0, 64) + jnp.where(popular, 0, 48)
    owner_index = jnp.arange(N_GZ, dtype=jnp.int32)
    owner_order = jnp.argsort(owner_score * N_GZ + owner_index, axis=-1, stable=True).astype(jnp.int32)
    slot_index = jnp.arange(slot_total, dtype=jnp.int32)
    slot_score = (jax.random.randint(key_slot, grid_shape + (slot_total,), 0, slot_total) + slot_index) * slot_total + slot_index
    slot_score = jnp.where(slot_index < SEND_CAP, slot_index - slot_total, slot_score)
    chosen = jnp.argsort(slot_score, axis=-1, stable=True)[..., :ITEMS].astype(jnp.int32)
    shuffle_score = jax.random.randint(key_shuffle, grid_shape + (ITEMS,), 0, 1 << 20) * ITEMS + jnp.arange(ITEMS, dtype=jnp.int32)
    shuffle = jnp.argsort(shuffle_score, axis=-1, stable=True).astype(jnp.int32)
    picked = jnp.take_along_axis(chosen, shuffle, axis=-1)
    bins = picked // SEND_CAP
    return jnp.take_along_axis(owner_order, bins, axis=-1).astype(jnp.int32)


def levels(key, dims, pieces, smallest, largest):
    def one(dim, shards_of):
        heights = jax.random.uniform(jax.random.fold_in(jax.random.fold_in(key, 6), dim), (shards_of,), jnp.float32, smallest / len(pieces), largest / len(pieces))
        return jnp.repeat(jnp.exp(heights), dims[dim] // shards_of).reshape((-1,) + (1,) * (len(dims) - dim - 1))

    factor_of = one(*pieces[0])
    for cut in pieces[1:]:
        factor_of = factor_of * one(*cut)
    return factor_of


def scatter_about(own_key, dims, scale, limit, pieces=(), kind=jnp.bfloat16):
    level = levels(own_key, dims, pieces, -0.22, 0.18) if pieces else 1.0
    entries = jax.random.normal(own_key, dims, jnp.float32) * scale * level
    return jnp.minimum(jnp.maximum(entries, -limit), limit).astype(kind)


def setup_inputs(seed: int = 0) -> dict:
    seeds = jax.random.split(jax.random.key(seed), 6)
    residual = scatter_about(seeds[0], (N_GX, N_GY, N_GZ, 3, FACE, R), 1.0, 6.0, ((0, 8), (1, 4), (2, 16)))
    face_basis = scatter_about(seeds[1], (N_GX, N_GY, N_GZ, 3, FACE, FACE), FACE ** -0.5, 0.375, ((0, 8), (1, 4), (2, 16)))
    factor = scatter_about(seeds[2], (N_GX, N_GY, N_GZ, SOLVE, SOLVE), SOLVE ** -0.5, 0.21875, ((0, 8), (1, 4), (2, 16)))
    coarse_inv = scatter_about(seeds[3], (N_GX, N_GY, N_GZ, CS, CS), CS ** -0.5, 0.21875, ((0, 8), (1, 4), (2, 16)))
    item_owner = draw_item_owner(jax.random.fold_in(seeds[5], 71), 0)
    return {"residual": residual, "face_basis": face_basis, "factor": factor, "coarse_inv": coarse_inv, "item_owner": item_owner}


def solve_twice(pair):
    matrix, vector = pair
    half_solve = lax.dot_general(matrix, vector, (((0,), (0,)), ((), ())), preferred_element_type=jnp.float32).astype(jnp.bfloat16)
    return jnp.dot(matrix, half_solve, preferred_element_type=jnp.float32).astype(jnp.bfloat16)


def coarse_apply(pair):
    matrix, vector = pair
    return lax.dot_general(matrix, vector, (((0,), (0,)), ((), ())), preferred_element_type=jnp.float32).astype(jnp.bfloat16)


def reference(residual, face_basis, factor, coarse_inv, item_owner):
    count = N_GX * N_GY * N_GZ
    transformed = jnp.einsum('xyzfac,xyzfar->xyzfcr', face_basis.astype(jnp.float32), residual.astype(jnp.float32))
    primal_items = transformed[:, :, :, :, :PF, :].astype(jnp.bfloat16).reshape(N_GX, N_GY, N_GZ, ITEMS, GROUP, R)
    dual_own = transformed[:, :, :, :, PF:, :].astype(jnp.bfloat16)
    dual_in = jnp.stack([jnp.roll(dual_own[:, :, :, 0], 1, axis=0), jnp.roll(dual_own[:, :, :, 1], 1, axis=1), jnp.roll(dual_own[:, :, :, 2], 1, axis=2)], axis=3)
    dual_load = (jnp.concatenate([dual_in, dual_own], axis=3) * 0.5).astype(jnp.bfloat16).reshape(count, SOLVE, R)
    solved = lax.map(solve_twice, (factor.reshape(count, SOLVE, SOLVE), dual_load)).reshape(N_GX, N_GY, N_GZ, 6, DF, R)
    lower_faces = solved[:, :, :, :3]
    upper_faces = solved[:, :, :, 3:]
    from_above = jnp.stack([jnp.roll(lower_faces[:, :, :, 0], -1, axis=0), jnp.roll(lower_faces[:, :, :, 1], -1, axis=1), jnp.roll(lower_faces[:, :, :, 2], -1, axis=2)], axis=3)
    dual_part = (0.5 * (upper_faces.astype(jnp.float32) + from_above.astype(jnp.float32))).astype(jnp.bfloat16)
    same_owner = item_owner[..., :, None] == item_owner[..., None, :]
    item_index = jnp.arange(ITEMS, dtype=jnp.int32)
    earlier = item_index[:, None] > item_index[None, :]
    slot_rank = jnp.sum((same_owner & earlier).astype(jnp.int32), axis=-1).astype(jnp.int32)
    gx_index = jnp.arange(N_GX, dtype=jnp.int32)[:, None, None, None]
    gy_index = jnp.arange(N_GY, dtype=jnp.int32)[None, :, None, None]
    gz_index = jnp.arange(N_GZ, dtype=jnp.int32)[None, None, :, None]
    holder = jnp.zeros((N_GX, N_GY, N_GZ, N_GZ, SEND_CAP, GROUP, R), jnp.bfloat16)
    holder = holder.at[gx_index, gy_index, item_owner, gz_index, slot_rank].set(primal_items)
    coarse_sol = lax.map(coarse_apply, (coarse_inv.reshape(count, CS, CS), holder.reshape(count, CS, R)))
    coarse_sol = coarse_sol.reshape(N_GX, N_GY, N_GZ, N_GZ, SEND_CAP, GROUP, R)
    primal_part = coarse_sol[gx_index, gy_index, item_owner, gz_index, slot_rank].reshape(N_GX, N_GY, N_GZ, 3, PF, R)
    combined = jnp.concatenate([primal_part, dual_part], axis=4)
    result = jnp.einsum('xyzfac,xyzfcr->xyzfar', face_basis.astype(jnp.float32), combined.astype(jnp.float32))
    return result.astype(jnp.bfloat16)
```

```python
import functools

import jax
import jax.numpy as jnp
from jax import lax
from jax.experimental import pallas as pl
from jax.experimental.pallas import tpu as pltpu
from jax.sharding import PartitionSpec as P

MESH = pl.DeviceIdType.MESH
PF = 128
GROUP = 16
ITEMS = 24
CAP = 3
NZ = 16
LANES = 128
BLOCK = CAP * GROUP
REACH = 4
DIRECT = 4

FAR = [(8, 0)] + [(d, s) for d in range(7, DIRECT, -1) for s in (1, -1)]
NEAR = [(d, s) for d in range(DIRECT, 0, -1) for s in (1, -1)]
ROUTES = FAR + NEAR

STEPS = (
    "slots",
    "primal0",
    "pack0",
    "barrier",
    "F0far",
    "F0near",
    "keep0",
    "dual",
    "up",
    "primal1",
    "pack1",
    "F1far",
    "keep1",
    "spread",
    "F0fwd",
    "F1near",
    "solve",
    "down",
    "ctrans",
    "F1fwd",
    "coarse0",
    "B0far",
    "B0near",
    "mean",
    "coarse1",
    "B1far",
    "B0fwd",
    "B1n43",
    "B1fwd",
    "B1n21",
    "final0",
    "final1",
)


def mod(value, n):
    return lax.rem(value + 4 * n, n)


def dot(a, b):
    return jnp.dot(a, b, preferred_element_type=jnp.float32)


def dot_nt(a, b):
    return lax.dot_general(a, b, (((1,), (1,)), ((), ())), preferred_element_type=jnp.float32)


def dot_t(a, b):
    return lax.dot_general(a, b, (((0,), (0,)), ((), ())), preferred_element_type=jnp.float32)


class Exchange:
    def __init__(self, me, src, dst, relay, send_sem, relay_sem, recv_sem, spare):
        self.me, self.src, self.dst, self.relay = me, src, dst, relay
        self.send_sem, self.relay_sem, self.recv_sem, self.spare = send_sem, relay_sem, recv_sem, spare

    def sign(self, s, upstream):
        return s if s else 1 - 2 * mod(self.me - upstream, 2)

    def copy(self, src, dst, recv_sem, target):
        return pltpu.make_async_remote_copy(
            src_ref=src, dst_ref=dst, send_sem=self.send_sem, recv_sem=recv_sem,
            device_id={"gz": target}, device_id_type=MESH)

    def send(self, routes):
        for d, s in routes:
            sg = self.sign(s, 0)
            src = self.src.at[mod(self.me + sg * d, NZ)]
            target = mod(self.me + sg * (REACH if d > DIRECT else d), NZ)
            if d > DIRECT:
                i = FAR.index((d, s))
                self.copy(src, self.relay.at[i], self.relay_sem.at[i], target).start()
            else:
                self.copy(src, self.dst.at[self.me], self.recv_sem, target).start()

    def forward(self, routes):
        for d, s in routes:
            i = FAR.index((d, s))
            sg = self.sign(s, REACH)
            held = self.relay.at[i]
            pltpu.make_async_copy(held, held, self.relay_sem.at[i]).wait()
            target = mod(self.me + sg * (d - REACH), NZ)
            self.copy(held, self.dst.at[mod(self.me - sg * REACH, NZ)], self.recv_sem, target).start()

    def keep_own(self):
        self.dst[self.me] = self.src[self.me]

    def arrive(self):
        got = self.spare.at[pl.ds(0, NZ - 1)]
        pltpu.make_async_copy(got, got, self.recv_sem).wait()

    def finish(self):
        sent = self.spare.at[pl.ds(0, len(ROUTES) + len(FAR))]
        pltpu.make_async_copy(sent, sent, self.send_sem).wait()


def kernel(resid_hbm, basis_hbm, factor_hbm, coarse_hbm, owner_hbm, out_ref,
           resid, basis, factor, coarse, coarse_t, owner, pick, spread, primal, extra, dual, dual_in, solved, above,
           pack, vec, sol, back, relay, spare, load_sem, send_sem, relay_sem, recv_sem, halo_send, halo_recv):
    gx, gy, gz = lax.axis_index("gx"), lax.axis_index("gy"), lax.axis_index("gz")
    axes = (("gx", gx), ("gy", gy), ("gz", gz))
    sizes = {name: lax.axis_size(name) for name, _ in axes}
    barrier = pltpu.get_barrier_semaphore()
    peers = [{name: mod(at + s, sizes[name])} for name, at in axes for s in (1, -1)]
    peers += [{"gz": mod(gz + s * h, NZ)} for h in range(2, DIRECT + 1) for s in (1, -1)]

    for peer in peers:
        pl.semaphore_signal(barrier, inc=1, device_id=peer, device_id_type=MESH)

    loads = [pltpu.make_async_copy(owner_hbm, owner, load_sem.at[0])]
    for src, dst in ((basis_hbm, basis), (resid_hbm, resid)):
        for f in range(3):
            loads.append(pltpu.make_async_copy(src.at[f], dst.at[f], load_sem.at[len(loads)]))
    for src, dst in ((factor_hbm, factor), (coarse_hbm, coarse)):
        loads.append(pltpu.make_async_copy(src, dst, load_sem.at[len(loads)]))
    for copy in loads:
        copy.start()

    def chunk(ch):
        return slice(ch * LANES, (ch + 1) * LANES)

    def slots():
        loads[0].wait()
        lane = lax.broadcasted_iota(jnp.int32, (1, ITEMS * GROUP), 1)
        item = lane // GROUP
        owners = [owner[i] for i in range(ITEMS)]
        mine = jnp.zeros_like(lane)
        for i in range(ITEMS):
            mine = jnp.where(item == i, owners[i], mine)
        rank = jnp.zeros_like(lane)
        for i in range(ITEMS):
            rank = rank + jnp.where((mine == owners[i]) & (item > i), 1, 0)
        place = (mine * CAP + rank) * GROUP + lax.rem(lane, GROUP)
        rows = lax.broadcasted_iota(jnp.int32, (NZ * BLOCK, ITEMS * GROUP), 0)
        pick[...] = jnp.where(rows == place, 1.0, 0.0).astype(jnp.bfloat16)

    def primal_rows(ch):
        for f in range(3):
            if ch == 0:
                loads[1 + f].wait()
                loads[4 + f].wait()
            t = dot_t(basis[f, :, :PF], resid[f, :, chunk(ch)])
            primal[f * PF:(f + 1) * PF, chunk(ch)] = t.astype(jnp.bfloat16)

    def pack_slots(ch):
        packed = dot(pick[...], primal[:, chunk(ch)]).astype(jnp.bfloat16)
        pack[ch] = packed.reshape(NZ, BLOCK, LANES)

    def dual_rows():
        for f in range(3):
            dual[f] = dot_t(basis[f, :, PF:], resid[f]).astype(jnp.bfloat16)

    def halo(src, dst, step, which):
        for k, (name, at) in enumerate(axes):
            pltpu.make_async_remote_copy(
                src_ref=src.at[k], dst_ref=dst.at[k], send_sem=halo_send.at[which], recv_sem=halo_recv.at[which],
                device_id={name: mod(at + step, sizes[name])}, device_id_type=MESH).start()

    def halo_wait(ref, sem):
        pltpu.make_async_copy(ref, ref, sem).wait()

    def solve():
        halo_wait(dual_in, halo_recv.at[0])
        loads[7].wait()
        halves = [(part[...] * 0.5).reshape(3 * PF, 2 * LANES) for part in (dual_in, dual)]
        load = jnp.concatenate(halves, axis=0).astype(jnp.bfloat16)
        half = dot_t(factor[...], load).astype(jnp.bfloat16)
        solved[...] = dot(factor[...], half).astype(jnp.bfloat16).reshape(6, PF, 2 * LANES)

    def mean():
        halo_wait(above, halo_recv.at[1])
        for k in range(3):
            half_sum = 0.5 * (solved[3 + k].astype(jnp.float32) + above[k].astype(jnp.float32))
            extra[k * 2 * PF:(k + 1) * 2 * PF, :] = dot(basis[k, :, PF:], half_sum.astype(jnp.bfloat16))

    def spread_basis():
        for f in range(3):
            columns = dot_nt(basis[f, :, :PF], pick[:, f * PF:(f + 1) * PF])
            spread[f * 2 * PF:(f + 1) * 2 * PF, :] = columns.astype(jnp.bfloat16)

    def ctrans():
        loads[8].wait()
        coarse_t[...] = coarse[...].T

    def exchange(which, ch, src, dst):
        return Exchange(gz, src.at[ch], dst.at[ch], relay.at[which, ch], send_sem.at[which, ch],
                        relay_sem.at[which, ch], recv_sem.at[which, ch], spare)

    trips = {("F", ch): exchange(0, ch, pack, vec) for ch in range(2)}
    trips |= {("B", ch): exchange(1, ch, sol, back) for ch in range(2)}

    def coarse_apply(ch):
        trips["F", ch].arrive()
        answer = dot(coarse_t[...], vec[ch].reshape(NZ * BLOCK, LANES)).astype(jnp.bfloat16)
        sol[ch] = answer.reshape(NZ, BLOCK, LANES)
        trips["B", ch].keep_own()

    def final(ch):
        trips["B", ch].arrive()
        total = dot(spread[...], back[ch].reshape(NZ * BLOCK, LANES)) + extra[:, chunk(ch)]
        out_ref[:, :, chunk(ch)] = total.astype(jnp.bfloat16).reshape(3, 2 * PF, LANES)

    run = {
        "slots": slots,
        "barrier": lambda: pl.semaphore_wait(barrier, len(peers)),
        "dual": dual_rows,
        "up": lambda: halo(dual, dual_in, 1, 0),
        "solve": solve,
        "down": lambda: halo(solved, above, -1, 1),
        "mean": mean,
        "ctrans": ctrans,
        "spread": spread_basis,
    }
    for ch in range(2):
        run[f"primal{ch}"] = functools.partial(primal_rows, ch)
        run[f"pack{ch}"] = functools.partial(pack_slots, ch)
        run[f"keep{ch}"] = trips["F", ch].keep_own
        run[f"coarse{ch}"] = functools.partial(coarse_apply, ch)
        run[f"final{ch}"] = functools.partial(final, ch)
        for way in "FB":
            trip = trips[way, ch]
            run[f"{way}{ch}far"] = functools.partial(trip.send, FAR)
            run[f"{way}{ch}near"] = functools.partial(trip.send, NEAR)
            run[f"{way}{ch}n43"] = functools.partial(trip.send, NEAR[:4])
            run[f"{way}{ch}n21"] = functools.partial(trip.send, NEAR[4:])
            run[f"{way}{ch}fwd"] = functools.partial(trip.forward, FAR)
            run[f"{way}{ch}fwA"] = functools.partial(trip.forward, FAR[:3])
            run[f"{way}{ch}fwB"] = functools.partial(trip.forward, FAR[3:])
    for step in STEPS:
        with jax.named_scope(step):
            run[step]()
    for trip in trips.values():
        trip.finish()
    halo_wait(dual_in, halo_send.at[0])
    halo_wait(above, halo_send.at[1])


def body(residual, face_basis, factor, coarse_inv, item_owner):
    bf16 = jnp.bfloat16
    blocks = pltpu.VMEM((2, NZ, BLOCK, LANES), bf16)
    faces = pltpu.VMEM((3, 2 * PF, 2 * LANES), bf16)
    halves = pltpu.VMEM((3, PF, 2 * LANES), bf16)
    square = pltpu.VMEM((NZ * BLOCK, NZ * BLOCK), bf16)
    table = pltpu.SMEM((ITEMS,), jnp.int32)
    semaphores = pltpu.SemaphoreType.DMA
    result = pl.pallas_call(
        kernel,
        out_shape=pltpu.VMEM((3, 2 * PF, 2 * LANES), bf16),
        in_specs=[pl.BlockSpec(memory_space=pltpu.HBM)] * 5,
        out_specs=pl.BlockSpec(memory_space=pltpu.VMEM),
        scratch_shapes=[
            faces, faces, square, square, square, table,
            pltpu.VMEM((NZ * BLOCK, ITEMS * GROUP), bf16), square,
            pltpu.VMEM((ITEMS * GROUP, 2 * LANES), bf16),
            pltpu.VMEM((NZ * BLOCK, 2 * LANES), jnp.float32),
            halves, halves, pltpu.VMEM((6, PF, 2 * LANES), bf16), halves,
            blocks, blocks, blocks, blocks,
            pltpu.VMEM((2, 2, len(FAR), BLOCK, LANES), bf16),
            pltpu.VMEM((len(ROUTES) + len(FAR), BLOCK, LANES), bf16),
            semaphores((9,)),
            semaphores((2, 2)), semaphores((2, 2, len(FAR))), semaphores((2, 2)), semaphores((2,)), semaphores((2,)),
        ],
        compiler_params=pltpu.CompilerParams(collective_id=0, has_side_effects=True, vmem_limit_bytes=60 * 1024 * 1024),
    )(residual[0, 0, 0], face_basis[0, 0, 0], factor[0, 0, 0], coarse_inv[0, 0, 0], item_owner[0, 0, 0])
    return result[None, None, None]


def solution(mesh):
    in_specs = (
        P("gx", "gy", "gz", None, None, None),
        P("gx", "gy", "gz", None, None, None),
        P("gx", "gy", "gz", None, None),
        P("gx", "gy", "gz", None, None),
        P("gx", "gy", "gz", None),
    )
    out_specs = P("gx", "gy", "gz", None, None, None)
    return jax.shard_map(body, mesh=mesh, in_specs=in_specs, out_specs=out_specs, check_vma=False)
```

```python
import functools

import jax
import jax.numpy as jnp
from jax import lax
from jax.experimental import pallas as pl
from jax.experimental.pallas import tpu as pltpu
from jax.sharding import PartitionSpec as P

MESH = pl.DeviceIdType.MESH
PF = 128
GROUP = 16
ITEMS = 24
CAP = 3
NZ = 16
LANES = 128
BLOCK = CAP * GROUP
DIRECT = 4
LEG = {8: 4, 7: 4, 6: 3, 5: 3}

FAR = [(8, 0)] + [(d, s) for d in range(7, DIRECT, -1) for s in (1, -1)]
NEAR = [(d, s) for d in range(DIRECT, 0, -1) for s in (1, -1)]
ROUTES = FAR + NEAR

STEPS = (
    "slots",
    "primal0",
    "pack0",
    "barrier",
    "F0far",
    "F0near",
    "keep0",
    "dual",
    "up",
    "primal1",
    "pack1",
    "F1far",
    "keep1",
    "spread",
    "F0fwA",
    "F1n43",
    "F0fwB",
    "F1n21",
    "solve",
    "down",
    "ctrans",
    "F1fwd",
    "coarse0",
    "B0far",
    "B0near",
    "mean",
    "coarse1",
    "B1far",
    "B0fwd",
    "B1n43",
    "B1fwA",
    "B1n21",
    "B1fwB",
    "final0",
    "final1",
)


def mod(value, n):
    return lax.rem(value + 4 * n, n)


def dot(a, b):
    return jnp.dot(a, b, preferred_element_type=jnp.float32)


def dot_nt(a, b):
    return lax.dot_general(a, b, (((1,), (1,)), ((), ())), preferred_element_type=jnp.float32)


def dot_t(a, b):
    return lax.dot_general(a, b, (((0,), (0,)), ((), ())), preferred_element_type=jnp.float32)


class Exchange:
    def __init__(self, me, src, dst, relay, send_sem, relay_sem, recv_sem, spare):
        self.me, self.src, self.dst, self.relay = me, src, dst, relay
        self.send_sem, self.relay_sem, self.recv_sem, self.spare = send_sem, relay_sem, recv_sem, spare

    def sign(self, s, upstream):
        return s if s else 1 - 2 * mod(self.me - upstream, 2)

    def copy(self, src, dst, recv_sem, target):
        return pltpu.make_async_remote_copy(
            src_ref=src, dst_ref=dst, send_sem=self.send_sem, recv_sem=recv_sem,
            device_id={"gz": target}, device_id_type=MESH)

    def send(self, routes):
        for d, s in routes:
            sg = self.sign(s, 0)
            src = self.src.at[mod(self.me + sg * d, NZ)]
            target = mod(self.me + sg * (LEG[d] if d > DIRECT else d), NZ)
            if d > DIRECT:
                i = FAR.index((d, s))
                self.copy(src, self.relay.at[i], self.relay_sem.at[i], target).start()
            else:
                self.copy(src, self.dst.at[self.me], self.recv_sem, target).start()

    def forward(self, routes):
        for d, s in routes:
            i = FAR.index((d, s))
            sg = self.sign(s, LEG[d])
            held = self.relay.at[i]
            pltpu.make_async_copy(held, held, self.relay_sem.at[i]).wait()
            target = mod(self.me + sg * (d - LEG[d]), NZ)
            self.copy(held, self.dst.at[mod(self.me - sg * LEG[d], NZ)], self.recv_sem, target).start()

    def keep_own(self):
        self.dst[self.me] = self.src[self.me]

    def arrive(self):
        got = self.spare.at[pl.ds(0, NZ - 1)]
        pltpu.make_async_copy(got, got, self.recv_sem).wait()

    def finish(self):
        sent = self.spare.at[pl.ds(0, len(ROUTES) + len(FAR))]
        pltpu.make_async_copy(sent, sent, self.send_sem).wait()


def kernel(resid_hbm, basis_hbm, factor_hbm, coarse_hbm, owner_hbm, out_ref,
           resid, basis, factor, coarse, coarse_t, owner, pick, spread, primal, extra, dual, dual_in, solved, above,
           pack, vec, sol, back, relay, spare, load_sem, send_sem, relay_sem, recv_sem, halo_send, halo_recv):
    gx, gy, gz = lax.axis_index("gx"), lax.axis_index("gy"), lax.axis_index("gz")
    axes = (("gx", gx), ("gy", gy), ("gz", gz))
    sizes = {name: lax.axis_size(name) for name, _ in axes}
    barrier = pltpu.get_barrier_semaphore()
    peers = [{"gz": mod(gz + s * h, NZ)} for h in range(DIRECT, 1, -1) for s in (1, -1)]
    peers += [{name: mod(at + s, sizes[name])} for name, at in axes[::-1] for s in (1, -1)]
    for peer in peers:
        pl.semaphore_signal(barrier, inc=1, device_id=peer, device_id_type=MESH)

    loads = [pltpu.make_async_copy(owner_hbm, owner, load_sem.at[0])]
    for src, dst in ((basis_hbm, basis), (resid_hbm, resid)):
        for f in range(3):
            loads.append(pltpu.make_async_copy(src.at[f], dst.at[f], load_sem.at[len(loads)]))
    for src, dst in ((factor_hbm, factor), (coarse_hbm, coarse)):
        loads.append(pltpu.make_async_copy(src, dst, load_sem.at[len(loads)]))
    for copy in loads:
        copy.start()

    def chunk(ch):
        return slice(ch * LANES, (ch + 1) * LANES)

    def slots():
        loads[0].wait()
        lane = lax.broadcasted_iota(jnp.int32, (1, ITEMS * GROUP), 1)
        item = lane // GROUP
        owners = [owner[i] for i in range(ITEMS)]
        mine = jnp.zeros_like(lane)
        for i in range(ITEMS):
            mine = jnp.where(item == i, owners[i], mine)
        rank = jnp.zeros_like(lane)
        for i in range(ITEMS):
            rank = rank + jnp.where((mine == owners[i]) & (item > i), 1, 0)
        place = (mine * CAP + rank) * GROUP + lax.rem(lane, GROUP)
        rows = lax.broadcasted_iota(jnp.int32, (NZ * BLOCK, ITEMS * GROUP), 0)
        pick[...] = jnp.where(rows == place, 1.0, 0.0).astype(jnp.bfloat16)

    def primal_rows(ch):
        for f in range(3):
            if ch == 0:
                loads[1 + f].wait()
                loads[4 + f].wait()
            t = dot_t(basis[f, :, :PF], resid[f, :, chunk(ch)])
            primal[f * PF:(f + 1) * PF, chunk(ch)] = t.astype(jnp.bfloat16)

    def pack_slots(ch):
        packed = dot(pick[...], primal[:, chunk(ch)]).astype(jnp.bfloat16)
        pack[ch] = packed.reshape(NZ, BLOCK, LANES)

    def dual_rows():
        for f in range(3):
            dual[f] = dot_t(basis[f, :, PF:], resid[f]).astype(jnp.bfloat16)

    def halo(src, dst, step, which):
        for k, (name, at) in enumerate(axes):
            pltpu.make_async_remote_copy(
                src_ref=src.at[k], dst_ref=dst.at[k], send_sem=halo_send.at[which], recv_sem=halo_recv.at[which],
                device_id={name: mod(at + step, sizes[name])}, device_id_type=MESH).start()

    def halo_wait(ref, sem):
        pltpu.make_async_copy(ref, ref, sem).wait()

    def solve():
        halo_wait(dual_in, halo_recv.at[0])
        loads[7].wait()
        halves = [(part[...] * 0.5).reshape(3 * PF, 2 * LANES) for part in (dual_in, dual)]
        load = jnp.concatenate(halves, axis=0).astype(jnp.bfloat16)
        half = dot_t(factor[...], load).astype(jnp.bfloat16)
        solved[...] = dot(factor[...], half).astype(jnp.bfloat16).reshape(6, PF, 2 * LANES)

    def mean():
        halo_wait(above, halo_recv.at[1])
        for k in range(3):
            half_sum = 0.5 * (solved[3 + k].astype(jnp.float32) + above[k].astype(jnp.float32))
            extra[k * 2 * PF:(k + 1) * 2 * PF, :] = dot(basis[k, :, PF:], half_sum.astype(jnp.bfloat16))

    def spread_basis():
        for f in range(3):
            columns = dot_nt(basis[f, :, :PF], pick[:, f * PF:(f + 1) * PF])
            spread[f * 2 * PF:(f + 1) * 2 * PF, :] = columns.astype(jnp.bfloat16)

    def ctrans():
        loads[8].wait()
        coarse_t[...] = coarse[...].T

    def exchange(which, ch, src, dst):
        return Exchange(gz, src.at[ch], dst.at[ch], relay.at[which, ch], send_sem.at[which, ch],
                        relay_sem.at[which, ch], recv_sem.at[which, ch], spare)

    trips = {("F", ch): exchange(0, ch, pack, vec) for ch in range(2)}
    trips |= {("B", ch): exchange(1, ch, sol, back) for ch in range(2)}

    def coarse_apply(ch):
        trips["F", ch].arrive()
        answer = dot(coarse_t[...], vec[ch].reshape(NZ * BLOCK, LANES)).astype(jnp.bfloat16)
        sol[ch] = answer.reshape(NZ, BLOCK, LANES)
        trips["B", ch].keep_own()

    def final(ch):
        trips["B", ch].arrive()
        total = dot(spread[...], back[ch].reshape(NZ * BLOCK, LANES)) + extra[:, chunk(ch)]
        out_ref[:, :, chunk(ch)] = total.astype(jnp.bfloat16).reshape(3, 2 * PF, LANES)

    run = {
        "slots": slots,
        "barrier": lambda: pl.semaphore_wait(barrier, len(peers)),
        "dual": dual_rows,
        "up": lambda: halo(dual, dual_in, 1, 0),
        "solve": solve,
        "down": lambda: halo(solved, above, -1, 1),
        "mean": mean,
        "ctrans": ctrans,
        "spread": spread_basis,
    }
    for ch in range(2):
        run[f"primal{ch}"] = functools.partial(primal_rows, ch)
        run[f"pack{ch}"] = functools.partial(pack_slots, ch)
        run[f"keep{ch}"] = trips["F", ch].keep_own
        run[f"coarse{ch}"] = functools.partial(coarse_apply, ch)
        run[f"final{ch}"] = functools.partial(final, ch)
        for way in "FB":
            trip = trips[way, ch]
            run[f"{way}{ch}far"] = functools.partial(trip.send, FAR)
            run[f"{way}{ch}near"] = functools.partial(trip.send, NEAR)
            run[f"{way}{ch}n43"] = functools.partial(trip.send, NEAR[:4])
            run[f"{way}{ch}n21"] = functools.partial(trip.send, NEAR[4:])
            run[f"{way}{ch}fwd"] = functools.partial(trip.forward, FAR)
            run[f"{way}{ch}fwA"] = functools.partial(trip.forward, FAR[:3])
            run[f"{way}{ch}fwB"] = functools.partial(trip.forward, FAR[3:])
    for step in STEPS:
        with jax.named_scope(step):
            run[step]()
    for trip in trips.values():
        trip.finish()
    halo_wait(dual_in, halo_send.at[0])
    halo_wait(above, halo_send.at[1])


def body(residual, face_basis, factor, coarse_inv, item_owner):
    bf16 = jnp.bfloat16
    blocks = pltpu.VMEM((2, NZ, BLOCK, LANES), bf16)
    faces = pltpu.VMEM((3, 2 * PF, 2 * LANES), bf16)
    halves = pltpu.VMEM((3, PF, 2 * LANES), bf16)
    square = pltpu.VMEM((NZ * BLOCK, NZ * BLOCK), bf16)
    table = pltpu.SMEM((ITEMS,), jnp.int32)
    semaphores = pltpu.SemaphoreType.DMA
    result = pl.pallas_call(
        kernel,
        out_shape=pltpu.VMEM((3, 2 * PF, 2 * LANES), bf16),
        in_specs=[pl.BlockSpec(memory_space=pltpu.HBM)] * 5,
        out_specs=pl.BlockSpec(memory_space=pltpu.VMEM),
        scratch_shapes=[
            faces, faces, square, square, square, table,
            pltpu.VMEM((NZ * BLOCK, ITEMS * GROUP), bf16), square,
            pltpu.VMEM((ITEMS * GROUP, 2 * LANES), bf16),
            pltpu.VMEM((NZ * BLOCK, 2 * LANES), jnp.float32),
            halves, halves, pltpu.VMEM((6, PF, 2 * LANES), bf16), halves,
            blocks, blocks, blocks, blocks,
            pltpu.VMEM((2, 2, len(FAR), BLOCK, LANES), bf16),
            pltpu.VMEM((len(ROUTES) + len(FAR), BLOCK, LANES), bf16),
            semaphores((9,)),
            semaphores((2, 2)), semaphores((2, 2, len(FAR))), semaphores((2, 2)), semaphores((2,)), semaphores((2,)),
        ],
        compiler_params=pltpu.CompilerParams(collective_id=0, has_side_effects=True, vmem_limit_bytes=60 * 1024 * 1024),
    )(residual[0, 0, 0], face_basis[0, 0, 0], factor[0, 0, 0], coarse_inv[0, 0, 0], item_owner[0, 0, 0])
    return result[None, None, None]


def solution(mesh):
    in_specs = (
        P("gx", "gy", "gz", None, None, None),
        P("gx", "gy", "gz", None, None, None),
        P("gx", "gy", "gz", None, None),
        P("gx", "gy", "gz", None, None),
        P("gx", "gy", "gz", None),
    )
    out_specs = P("gx", "gy", "gz", None, None, None)
    return jax.shard_map(body, mesh=mesh, in_specs=in_specs, out_specs=out_specs, check_vma=False)
```
